32 devices in a mesh: section: 4 (over y, x), dp: 8 (over z, core).
Axes of the slice: x: 2, y: 2, z: 4, core: 2. Of those that a mesh axis runs over, the one named last changes fastest.
Arguments:
- activations: bfloat16 [4, 8, 257, 1792], P('section', 'dp'), may hold values from -6 to 6
- saved: bfloat16 [4, 8, 257, 1792], P('section', 'dp'), may hold values from -6 to 6
- cotangents: bfloat16 [4, 8, 257, 1792], P('section', 'dp'), may hold values from -1.1953125 to 1.1953125
- projection: bfloat16 [4, 1792, 1792], P('section'), may hold values from -0.125 to 0.125
- section_gain: float32 [4, 1792], P('section'), may hold values from 0.5 to 1.5
- final_gain: float32 [1792], replicated, may hold values from 0.5 to 1.5
- head_weight: bfloat16 [1792, 1024], P('section'), may hold values from -0.125 to 0.125
- text_embed: bfloat16 [8, 1024], P('dp'), may hold values from -6 to 6
- labels: int32 [8], P('dp'), may hold values from 0 to 7, each once
Outputs:
- next_act: bfloat16 [4, 8, 257, 1792], P('section', 'dp')
- next_grad: bfloat16 [4, 8, 257, 1792], P('section', 'dp')
- mean_loss: float32 [4], P('section')
The draws below stay inside these ranges and needn't reach their ends.
Inputs may be any that keep to these rules, and one draw needn't show every extreme that they name: labels holds each caption index once.
All inputs are finite; a program needn't handle non-finite values.
Results may differ from the reference program's by a relative error of at most 0.0039.
Values may be sent and summed in bfloat16 or wider, within the bound.
A program may use at most 64 MiB of HBM per device.

```python
import jax
import jax.numpy as jnp
from jax import lax

D = 1792
E = 1024
TOK = 257
B = 8
N_SECTION = 4


def block_scale(key, extent, split, low, high):
    def one(position, shards_of):
        draws = jax.random.uniform(jax.random.fold_in(jax.random.fold_in(key, 6), position), (shards_of,), jnp.float32, low / len(split), high / len(split))
        return jnp.repeat(jnp.exp(draws), extent[position] // shards_of).reshape((-1,) + (1,) * (len(extent) - position - 1))

    factor_of = one(*split[0])
    for cut in split[1:]:
        factor_of = factor_of * one(*cut)
    return factor_of


def noise(key, dims, width, most, cuts=(), held_as=jnp.bfloat16):
    array = width * jax.random.normal(key, dims, jnp.float32)
    if cuts:
        array = array * block_scale(key, dims, cuts, -0.22, 0.18)
    return jnp.clip(array, -most, most).astype(held_as)


def setup_inputs(seed: int = 0) -> dict:
    arg_keys = jax.random.split(jax.random.key(seed), 10)
    return {
        "activations": noise(arg_keys[0], (N_SECTION, B, TOK, D), 1.0, 6.0, ((0, 4), (1, 8))),
        "saved": noise(arg_keys[1], (N_SECTION, B, TOK, D), 1.0, 6.0, ((0, 4), (1, 8))),
        "cotangents": noise(arg_keys[2], (N_SECTION, B, TOK, D), 0.2, 1.1953125, ((0, 4), (1, 8))),
        "projection": noise(arg_keys[3], (N_SECTION, D, D), D ** -0.5, 0.125, ((0, 4),)),
        "section_gain": jnp.clip(1.0 + 0.1 * jax.random.normal(arg_keys[4], (N_SECTION, D), jnp.float32), 0.5, 1.5),
        "final_gain": jnp.clip(1.0 + 0.1 * jax.random.normal(arg_keys[5], (D,), jnp.float32), 0.5, 1.5),
        "head_weight": noise(arg_keys[6], (D, E), D ** -0.5, 0.125, ((0, 4),)),
        "text_embed": noise(arg_keys[7], (B, E), 1.0, 6.0, ((0, 8),)),
        "labels": jax.random.permutation(arg_keys[8], B).astype(jnp.int32),
    }


epsilon = 1e-06
logit_scale = 100.0

def norm_rows(values):
    centre = lax.optimization_barrier(jnp.mean(values, axis=-1, keepdims=True))
    centred = values - centre
    variance = lax.optimization_barrier(jnp.mean(centred * centred, axis=-1, keepdims=True))
    inverse = lax.rsqrt(variance + epsilon)
    return (centred * inverse, inverse)

def unit_rows(values):
    inverse = lax.rsqrt(lax.optimization_barrier(jnp.sum(values * values, axis=-1, keepdims=True)) + epsilon)
    return (values * inverse, inverse)

def forward_block(block_in, weight, scale_row):
    block_shape = block_in.shape
    standard, inverse = norm_rows(block_in.astype(jnp.float32))
    normed = (standard * scale_row).astype(jnp.bfloat16)
    mixed = jnp.dot(normed.reshape(-1, block_shape[-1]), weight, preferred_element_type=jnp.float32)
    return (block_in.astype(jnp.float32) + mixed.reshape(block_shape)).astype(jnp.bfloat16)

def backward_block(cotangent, restored, weight, scale_row):
    block_shape = restored.shape
    standard, inverse = norm_rows(restored.astype(jnp.float32))
    d_normed = lax.dot_general(cotangent.reshape(-1, block_shape[-1]), weight, (((1,), (1,)), ((), ())), preferred_element_type=jnp.float32).reshape(block_shape)
    d_standard = d_normed * scale_row
    d_input = cotangent.astype(jnp.float32) + inverse * (d_standard - lax.optimization_barrier(jnp.mean(d_standard, axis=-1, keepdims=True)) - standard * lax.optimization_barrier(jnp.mean(d_standard * standard, axis=-1, keepdims=True)))
    return d_input.astype(jnp.bfloat16)

def reference(activations, saved, cotangents, projection, section_gain, final_gain, head_weight, text_embed, labels):
    block_out = lax.map(lambda item: forward_block(item[0], item[1], item[2]), (activations, projection, section_gain))
    last_out = block_out[-1]
    pooled = lax.optimization_barrier(jnp.mean(last_out.astype(jnp.float32), axis=1))
    pooled_std, pooled_inv = norm_rows(pooled)
    pooled_norm = (pooled_std * final_gain).astype(jnp.bfloat16)
    embedding = jnp.dot(pooled_norm, head_weight, preferred_element_type=jnp.float32)
    image_unit, image_inv = unit_rows(embedding)
    text_unit, text_inv = unit_rows(text_embed.astype(jnp.float32))
    logits = logit_scale * jnp.dot(image_unit, text_unit.T, precision=lax.Precision.HIGHEST)
    count = logits.shape[0]
    targets = (labels[:, None] == jnp.arange(count, dtype=jnp.int32)[None, :]).astype(jnp.float32)
    row_lse = jax.nn.logsumexp(logits, axis=1)
    col_lse = jax.nn.logsumexp(logits, axis=0)
    picked = lax.optimization_barrier(jnp.sum(logits * targets, axis=1))
    col_picked = lax.optimization_barrier(jnp.sum(col_lse[None, :] * targets, axis=1))
    loss_value = 0.5 * jnp.mean(row_lse - picked) + 0.5 * jnp.mean(col_picked - picked)
    section_count = activations.shape[0]
    mean_loss = jnp.zeros((section_count,), jnp.float32).at[-1].set(loss_value)
    row_prob = jnp.exp(logits - row_lse[:, None])
    col_prob = jnp.exp(logits - col_lse[None, :])
    d_logits = 0.5 * (row_prob - targets + (col_prob - targets))
    d_image = logit_scale * jnp.dot(d_logits, text_unit, precision=lax.Precision.HIGHEST)
    d_embedding = (d_image - image_unit * lax.optimization_barrier(jnp.sum(d_image * image_unit, axis=-1, keepdims=True))) * image_inv
    d_pooled_norm = lax.dot_general(d_embedding.astype(jnp.bfloat16), head_weight, (((1,), (1,)), ((), ())), preferred_element_type=jnp.float32)
    d_std = d_pooled_norm * final_gain
    d_pooled = pooled_inv * (d_std - lax.optimization_barrier(jnp.mean(d_std, axis=-1, keepdims=True)) - pooled_std * lax.optimization_barrier(jnp.mean(d_std * pooled_std, axis=-1, keepdims=True)))
    loss_grad = jnp.broadcast_to((d_pooled / TOK)[:, None, :], last_out.shape).astype(jnp.bfloat16)
    d_input = lax.map(lambda item: backward_block(item[0], item[1], item[2], item[3]), (cotangents, saved, projection, section_gain))
    next_act = jnp.concatenate([jnp.zeros_like(block_out[:1]), block_out[:-1]], axis=0)
    next_grad = jnp.concatenate([d_input[1:], loss_grad[None]], axis=0)
    return (next_act, next_grad, mean_loss)
```

```python
import functools

import jax
import jax.numpy as jnp
from jax import lax
from jax.experimental import pallas as pl
from jax.experimental.pallas import tpu as pltpu
from jax.sharding import PartitionSpec as P

epsilon = 1e-06
logit_scale = 100.0


def shifted(value, axis, steps):
    count = lax.axis_size(axis)
    first, last = (max(0, -steps), min(count, count - steps))
    return lax.ppermute(value, axis, [(source, source + steps) for source in range(first, last)])


def norm_rows(values):
    centre = jnp.mean(values, axis=-1, keepdims=True)
    centred = values - centre
    variance = jnp.mean(centred * centred, axis=-1, keepdims=True)
    inverse = lax.rsqrt(variance + epsilon)
    return (centred * inverse, inverse)


def forward_block(block_in, weight, scale_row):
    block_shape = block_in.shape
    standard, inverse = norm_rows(block_in.astype(jnp.float32))
    normed = (standard * scale_row).astype(jnp.bfloat16)
    mixed = jnp.dot(normed.reshape(-1, block_shape[-1]), weight, preferred_element_type=jnp.float32)
    return (block_in.astype(jnp.float32) + mixed.reshape(block_shape)).astype(jnp.bfloat16)


def backward_block(cotangent, restored, weight, scale_row):
    block_shape = restored.shape
    standard, inverse = norm_rows(restored.astype(jnp.float32))
    d_normed = lax.dot_general(
        cotangent.reshape(-1, block_shape[-1]),
        weight,
        (((1,), (1,)), ((), ())),
        preferred_element_type=jnp.float32,
    ).reshape(block_shape)
    d_standard = d_normed * scale_row
    d_input = cotangent.astype(jnp.float32) + inverse * (
        d_standard
        - jnp.mean(d_standard, axis=-1, keepdims=True)
        - standard * jnp.mean(d_standard * standard, axis=-1, keepdims=True)
    )
    return d_input.astype(jnp.bfloat16)


MESH = pl.DeviceIdType.MESH


def exchange(slots, send, recv, axis, me, peers):
    def start(step, carry):
        peer = lax.rem(me + step, peers)
        pltpu.make_async_remote_copy(
            slots.at[me], slots.at[me], send.at[peer], recv.at[me], {axis: peer}, MESH
        ).start()
        return carry

    lax.fori_loop(1, peers, start, 0)


def arrived(slots, send, recv, axis, me, peers):
    def wait(step, carry):
        peer = lax.rem(me + step, peers)
        pltpu.make_async_remote_copy(
            slots.at[me], slots.at[peer], send.at[peer], recv.at[peer], {axis: peer}, MESH
        ).wait_recv()
        return carry

    lax.fori_loop(1, peers, wait, 0)


def sent(slots, send, recv, axis, me, peers):
    def wait(step, carry):
        peer = lax.rem(me + step, peers)
        pltpu.make_async_remote_copy(
            slots.at[me], slots.at[me], send.at[peer], recv.at[peer], {axis: peer}, MESH
        ).wait_send()
        return carry

    lax.fori_loop(1, peers, wait, 0)


def enter(sections, replicas):
    section, replica = lax.axis_index("section"), lax.axis_index("dp")
    barrier = pltpu.get_barrier_semaphore()

    def greet_section(step, carry):
        peer = lax.rem(section + step, sections)
        pl.semaphore_signal(barrier, inc=1, device_id={"section": peer}, device_id_type=MESH)
        return carry

    def greet_replica(step, carry):
        peer = lax.rem(replica + step, replicas)
        pl.semaphore_signal(barrier, inc=1, device_id={"dp": peer}, device_id_type=MESH)
        return carry

    lax.fori_loop(1, sections, greet_section, 0)
    lax.fori_loop(1, replicas, greet_replica, 0)
    pl.semaphore_wait(barrier, sections + replicas - 2)


def total_mean(pieces, width):
    return jnp.sum(jnp.sum(pieces, axis=2, keepdims=True), axis=0, keepdims=True) / width


def loss_chain(
    sections,
    replicas,
    tokens,
    pooled_ref,
    gain_ref,
    head_ref,
    text_ref,
    label_ref,
    grad_ref,
    loss_ref,
    feats,
    feat_in,
    parts,
    images,
    texts,
    back,
    feat_send,
    feat_recv,
    part_send,
    part_recv,
    image_send,
    image_recv,
    text_send,
    text_recv,
    back_send,
    back_recv,
):
    section, replica = lax.axis_index("section"), lax.axis_index("dp")
    last = sections - 1
    rows = pooled_ref.shape[2]
    width = sections * rows
    span = text_ref.shape[1]
    text = text_ref[...].astype(jnp.float32)
    text_inv = lax.rsqrt(jnp.sum(text * text, axis=-1, keepdims=True) + epsilon)
    texts[replica, :, 0:span] = text * text_inv
    texts[replica, :, span:] = label_ref[...]
    pooled = pooled_ref[...]
    centred = pooled - total_mean(pooled, width)
    pooled_inv = lax.rsqrt(total_mean(centred * centred, width) + epsilon)
    pooled_std = centred * pooled_inv
    feats[...] = (pooled_std * gain_ref[...]).astype(jnp.bfloat16).astype(jnp.float32)
    enter(sections, replicas)

    @pl.when(section == last)
    def _():
        for peer in range(last):
            pltpu.make_async_remote_copy(
                feats.at[peer], feat_in, feat_send.at[peer], feat_recv, {"section": peer}, MESH
            ).start()
        feat_in[...] = feats[last]

    exchange(texts, text_send, text_recv, "dp", replica, replicas)

    @pl.when(section != last)
    def _():
        pltpu.make_async_remote_copy(
            feats.at[0], feat_in, feat_send.at[0], feat_recv, {"section": last}, MESH
        ).wait_recv()

    parts[section] = jnp.dot(
        feat_in[...].astype(jnp.bfloat16), head_ref[...], preferred_element_type=jnp.float32
    )
    exchange(parts, part_send, part_recv, "section", section, sections)
    arrived(texts, text_send, text_recv, "dp", replica, replicas)
    arrived(parts, part_send, part_recv, "section", section, sections)
    embedding = jnp.sum(parts[...], axis=0)
    image_inv = lax.rsqrt(jnp.sum(embedding * embedding, axis=-1, keepdims=True) + epsilon)
    image_unit = embedding * image_inv
    images[replica] = image_unit
    exchange(images, image_send, image_recv, "dp", replica, replicas)
    all_text = texts[:, 0, 0:span]
    label_column = texts[:, 0, span : span + 1]
    column = lax.broadcasted_iota(jnp.int32, (replicas, replicas), 1)
    row = lax.broadcasted_iota(jnp.int32, (replicas, replicas), 0)
    targets = jnp.where(label_column == column.astype(jnp.float32), 1.0, 0.0)
    arrived(images, image_send, image_recv, "dp", replica, replicas)
    all_image = images[:, 0, :]
    logits = logit_scale * lax.dot_general(
        all_image,
        all_text,
        (((1,), (1,)), ((), ())),
        precision=lax.Precision.HIGHEST,
        preferred_element_type=jnp.float32,
    )
    row_max = jnp.max(logits, axis=1, keepdims=True)
    row_lse = row_max + jnp.log(jnp.sum(jnp.exp(logits - row_max), axis=1, keepdims=True))
    col_max = jnp.max(logits, axis=0, keepdims=True)
    col_lse = col_max + jnp.log(jnp.sum(jnp.exp(logits - col_max), axis=0, keepdims=True))
    d_logits = 0.5 * ((jnp.exp(logits - row_lse) - targets) + (jnp.exp(logits - col_lse) - targets))
    own = jnp.sum(jnp.where(row == replica, d_logits, 0.0), axis=0, keepdims=True)
    d_image = logit_scale * jnp.dot(
        own, all_text, precision=lax.Precision.HIGHEST, preferred_element_type=jnp.float32
    )
    along = jnp.sum(d_image * image_unit, axis=-1, keepdims=True)
    d_embedding = ((d_image - image_unit * along) * image_inv).astype(jnp.bfloat16)
    back[section] = lax.dot_general(
        d_embedding,
        head_ref[...],
        (((1,), (1,)), ((), ())),
        preferred_element_type=jnp.float32,
    )

    @pl.when(section != last)
    def _():
        pltpu.make_async_remote_copy(
            back.at[section], back.at[section], back_send, back_recv.at[section], {"section": last}, MESH
        ).start()

    picked = jnp.sum(logits * targets, axis=1, keepdims=True)
    col_picked = jnp.sum(col_lse * targets, axis=1, keepdims=True)
    loss = 0.5 * (row_lse - picked) + 0.5 * (col_picked - picked)
    loss_ref[...] = jnp.broadcast_to(jnp.sum(loss, axis=0, keepdims=True) / replicas, loss_ref.shape)

    @pl.when(section == last)
    def _():
        for peer in range(last):
            pltpu.make_async_remote_copy(
                back.at[peer], back.at[peer], back_send, back_recv.at[peer], {"section": peer}, MESH
            ).wait_recv()

    d_std = back[...] * gain_ref[...]
    d_pooled = pooled_inv * (
        d_std - total_mean(d_std, width) - pooled_std * total_mean(d_std * pooled_std, width)
    )
    grad_ref[...] = d_pooled / tokens
    sent(texts, text_send, text_recv, "dp", replica, replicas)
    sent(images, image_send, image_recv, "dp", replica, replicas)
    sent(parts, part_send, part_recv, "section", section, sections)

    @pl.when(section == last)
    def _():
        for peer in range(last):
            pltpu.make_async_remote_copy(
                feats.at[peer], feat_in, feat_send.at[peer], feat_recv, {"section": peer}, MESH
            ).wait_send()

    @pl.when(section != last)
    def _():
        pltpu.make_async_remote_copy(
            back.at[section], back.at[section], back_send, back_recv.at[section], {"section": last}, MESH
        ).wait_send()


def run_chain(pooled, gain, head_weight, text, labels, tokens):
    sections, replicas = lax.axis_size("section"), lax.axis_size("dp")
    rows, span = head_weight.shape
    label_row = jnp.broadcast_to(labels.astype(jnp.float32)[:, None], (1, 128))
    f32 = jnp.float32
    dma = pltpu.SemaphoreType.DMA
    vmem = pl.BlockSpec(memory_space=pltpu.VMEM)
    return pl.pallas_call(
        functools.partial(loss_chain, sections, replicas, tokens),
        out_shape=(
            jax.ShapeDtypeStruct((sections, 1, rows), f32),
            jax.ShapeDtypeStruct((1, 128), f32),
        ),
        in_specs=[vmem] * 5,
        out_specs=(vmem, vmem),
        scratch_shapes=[
            pltpu.VMEM((sections, 1, rows), f32),
            pltpu.VMEM((1, rows), f32),
            pltpu.VMEM((sections, 1, span), f32),
            pltpu.VMEM((replicas, 1, span), f32),
            pltpu.VMEM((replicas, 1, span + 128), f32),
            pltpu.VMEM((sections, 1, rows), f32),
            dma((sections,)),
            dma,
            dma((sections,)),
            dma((sections,)),
            dma((replicas,)),
            dma((replicas,)),
            dma((replicas,)),
            dma((replicas,)),
            dma,
            dma((sections,)),
        ],
        compiler_params=pltpu.CompilerParams(collective_id=0, has_side_effects=True),
        cost_estimate=pl.CostEstimate(flops=100000000, bytes_accessed=1000000, transcendentals=0),
        name="loss_chain",
    )(
        pooled.reshape(sections, 1, rows),
        gain.reshape(sections, 1, rows),
        head_weight,
        text,
        label_row,
    )


def local(
    activations,
    saved,
    cotangents,
    projection,
    section_gain,
    final_gain,
    head_weight,
    text_embed,
    labels,
):
    sections = lax.axis_size("section")
    is_last = lax.axis_index("section") == sections - 1
    weight = projection[0]
    scale_row = section_gain[0]
    block_out = forward_block(activations[0], weight, scale_row)
    next_act = shifted(block_out[None], "section", 1)
    d_input = backward_block(cotangents[0], saved[0], weight, scale_row)
    passed_grad = shifted(d_input[None], "section", -1)
    pooled = jnp.mean(block_out.astype(jnp.float32), axis=1)
    grad_row, loss_row = run_chain(
        pooled, final_gain, head_weight, text_embed, labels, block_out.shape[1]
    )
    loss_grad = jnp.broadcast_to(
        grad_row.reshape(1, 1, -1).astype(jnp.bfloat16), block_out.shape
    )
    next_grad = jnp.where(is_last, loss_grad[None], passed_grad)
    mean_loss = jnp.where(is_last, loss_row[0, 0], jnp.float32(0.0))[None]
    return (next_act, next_grad, mean_loss)


def solution(mesh):
    return jax.shard_map(
        local,
        mesh=mesh,
        in_specs=(
            P("section", "dp", None, None),
            P("section", "dp", None, None),
            P("section", "dp", None, None),
            P("section", None, None),
            P("section", None),
            P(),
            P("section", None),
            P("dp", None),
            P("dp"),
        ),
        out_specs=(P("section", "dp", None, None), P("section", "dp", None, None), P("section")),
        check_vma=False,
    )
```

```python
import functools
import math

import jax
import jax.numpy as jnp
from jax import lax
from jax.experimental import pallas as pl
from jax.experimental.pallas import tpu as pltpu
from jax.sharding import PartitionSpec as P

epsilon = 1e-06
logit_scale = 100.0
MESH = pl.DeviceIdType.MESH


def exchange(slots, send, recv, axis, me, peers):
    def start(step, carry):
        peer = lax.rem(me + step, peers)
        pltpu.make_async_remote_copy(
            slots.at[me], slots.at[me], send.at[peer], recv.at[me], {axis: peer}, MESH
        ).start()
        return carry

    lax.fori_loop(1, peers, start, 0)


def arrived(slots, send, recv, axis, me, peers):
    def wait(step, carry):
        peer = lax.rem(me + step, peers)
        pltpu.make_async_remote_copy(
            slots.at[me], slots.at[peer], send.at[peer], recv.at[peer], {axis: peer}, MESH
        ).wait_recv()
        return carry

    lax.fori_loop(1, peers, wait, 0)


def sent(slots, send, recv, axis, me, peers):
    def wait(step, carry):
        peer = lax.rem(me + step, peers)
        pltpu.make_async_remote_copy(
            slots.at[me], slots.at[me], send.at[peer], recv.at[peer], {axis: peer}, MESH
        ).wait_send()
        return carry

    lax.fori_loop(1, peers, wait, 0)


def enter(sections, replicas):
    section, replica = lax.axis_index("section"), lax.axis_index("dp")
    barrier = pltpu.get_barrier_semaphore()

    def greet_section(step, carry):
        peer = lax.rem(section + step, sections)
        pl.semaphore_signal(barrier, inc=1, device_id={"section": peer}, device_id_type=MESH)
        return carry

    def greet_replica(step, carry):
        peer = lax.rem(replica + step, replicas)
        pl.semaphore_signal(barrier, inc=1, device_id={"dp": peer}, device_id_type=MESH)
        return carry

    lax.fori_loop(1, sections, greet_section, 0)
    lax.fori_loop(1, replicas, greet_replica, 0)
    pl.semaphore_wait(barrier, sections + replicas - 2)


def row_stats(values):
    width = values.shape[-1]
    centre = jnp.sum(values, axis=-1, keepdims=True) / width
    centred = values - centre
    variance = jnp.sum(centred * centred, axis=-1, keepdims=True) / width
    return centre, lax.rsqrt(variance + epsilon)


def step_kernel(
    sections,
    replicas,
    group,
    chunk,
    act_ref,
    saved_ref,
    cot_ref,
    weight_ref,
    head_ref,
    scale_ref,
    gain_ref,
    text_ref,
    label_ref,
    next_ref,
    grad_ref,
    loss_ref,
    act,
    saved,
    cot,
    weight,
    normed,
    block,
    d_input,
    slope,
    pooled,
    heads,
    feats,
    columns,
    images,
    texts,
    d_rows,
    part_out,
    part_in,
    load_sem,
    weight_sem,
    head_send,
    head_recv,
    fwd_send,
    fwd_recv,
    bwd_send,
    bwd_recv,
    fill_sem,
    feat_send,
    feat_recv,
    col_send,
    col_recv,
    image_send,
    image_recv,
    text_send,
    text_recv,
    part_send,
    part_recv,
):
    section, replica = lax.axis_index("section"), lax.axis_index("dp")
    last = sections - 1
    tokens, width = act.shape
    rows, span = head_ref.shape
    shards = width // chunk
    slot = lax.rem(replica, group)
    first = replica - slot
    shard = span // group
    f32, bf16 = jnp.float32, jnp.bfloat16

    def cut(index):
        return pl.ds(pl.multiple_of(index * chunk, chunk), chunk)

    def weight_load(index):
        return pltpu.make_async_copy(
            weight_ref.at[:, cut(index)], weight.at[:, cut(index)], weight_sem.at[index]
        )

    load_act = pltpu.make_async_copy(act_ref, act, load_sem.at[0])
    load_saved = pltpu.make_async_copy(saved_ref, saved, load_sem.at[1])
    load_cot = pltpu.make_async_copy(cot_ref, cot, load_sem.at[2])
    load_act.start()
    for index in range(shards):
        weight_load(index).start()
    load_saved.start()
    load_cot.start()
    enter(sections, replicas)

    my_columns = pl.ds(pl.multiple_of(slot * shard, shard), shard)

    def head_rows(owner):
        return pl.ds(pl.multiple_of(owner * rows, rows), rows)

    def head_copy(owner):
        return pltpu.make_async_remote_copy(
            head_ref.at[:, my_columns],
            heads.at[head_rows(owner), :],
            head_send,
            head_recv.at[owner],
            {"section": last},
            MESH,
        )

    own_head = pltpu.make_async_copy(
        head_ref.at[:, my_columns], heads.at[head_rows(last), :], head_send
    )

    @pl.when(section < last)
    def _():
        head_copy(section).start()

    @pl.when(section == last)
    def _():
        own_head.start()
        text = text_ref[...].astype(f32)
        text_inv = lax.rsqrt(jnp.sum(text * text, axis=-1, keepdims=True) + epsilon)
        texts[replica, :, 0:span] = text * text_inv
        texts[replica, :, span:] = label_ref[...]
        exchange(texts, text_send, text_recv, "dp", replica, replicas)

    load_act.wait()
    values = act[...].astype(f32)
    centre, inverse = row_stats(values)
    normed[...] = ((values - centre) * inverse * scale_ref[...]).astype(bf16)

    def forward_copy(index):
        return pltpu.make_async_remote_copy(
            block.at[:, cut(index)],
            next_ref.at[:, cut(index)],
            fwd_send.at[index],
            fwd_recv.at[index],
            {"section": section + 1},
            MESH,
        )

    def backward_copy(index):
        return pltpu.make_async_remote_copy(
            d_input.at[:, cut(index)],
            grad_ref.at[:, cut(index)],
            bwd_send.at[index],
            bwd_recv.at[index],
            {"section": section - 1},
            MESH,
        )

    def forward_step(index, carry):
        weight_load(index).wait()
        mixed = jnp.dot(normed[...], weight[:, cut(index)], preferred_element_type=f32)
        piece = (act[:, cut(index)].astype(f32) + mixed).astype(bf16)
        block[:, cut(index)] = piece
        pooled[:, cut(index)] = jnp.sum(piece.astype(f32), axis=0, keepdims=True) / tokens

        @pl.when(section < last)
        def _():
            forward_copy(index).start()

        return carry

    lax.fori_loop(0, shards, forward_step, 0)
    load_saved.wait()
    load_cot.wait()

    @pl.when(section > 0)
    def _():
        centre, inverse = row_stats(saved[...].astype(f32))

        def gradient_step(index, carry):
            sum_slope, sum_product = carry
            d_normed = lax.dot_general(
                cot[...],
                weight[cut(index), :],
                (((1,), (1,)), ((), ())),
                preferred_element_type=f32,
            )
            piece = d_normed * scale_ref[:, cut(index)]
            standard = (saved[:, cut(index)].astype(f32) - centre) * inverse
            slope[:, cut(index)] = piece
            return (
                sum_slope + jnp.sum(piece, axis=-1, keepdims=True),
                sum_product + jnp.sum(piece * standard, axis=-1, keepdims=True),
            )

        zero = jnp.zeros((tokens, 1), f32)
        sum_slope, sum_product = lax.fori_loop(0, shards, gradient_step, (zero, zero))
        mean_slope, mean_product = sum_slope / width, sum_product / width

        def emit_step(index, carry):
            standard = (saved[:, cut(index)].astype(f32) - centre) * inverse
            d_input[:, cut(index)] = (
                cot[:, cut(index)].astype(f32)
                + inverse * (slope[:, cut(index)] - mean_slope - standard * mean_product)
            ).astype(bf16)
            backward_copy(index).start()
            return carry

        lax.fori_loop(0, shards, emit_step, 0)

    loss_ref[...] = jnp.zeros_like(loss_ref)

    fill_next = pltpu.make_async_copy(normed, next_ref, fill_sem)
    fill_grad = pltpu.make_async_copy(block, grad_ref, fill_sem)

    @pl.when(section == 0)
    def _():
        normed[...] = jnp.zeros_like(normed)
        fill_next.start()
        fill_next.wait()

    @pl.when(section == last)
    def _():
        mean_row = pooled[...]
        centre, pooled_inv = row_stats(mean_row)
        pooled_std = (mean_row - centre) * pooled_inv
        feats[slot] = (pooled_std * gain_ref[...]).astype(bf16).astype(f32)

        def in_group(make):
            def go(step, carry):
                peer = lax.rem(slot + step, group)
                make(peer)
                return carry

            lax.fori_loop(1, group, go, 0)

        def feat_copy(peer, source):
            return pltpu.make_async_remote_copy(
                feats.at[slot],
                feats.at[source],
                feat_send.at[peer],
                feat_recv.at[source],
                {"dp": first + peer},
                MESH,
            )

        def col_copy(peer, source):
            return pltpu.make_async_remote_copy(
                columns.at[slot],
                columns.at[source],
                col_send.at[peer],
                col_recv.at[source],
                {"dp": first + peer},
                MESH,
            )

        def part_copy(peer, source):
            return pltpu.make_async_remote_copy(
                part_out.at[peer],
                part_in.at[source],
                part_send.at[peer],
                part_recv.at[source],
                {"dp": first + peer},
                MESH,
            )

        in_group(lambda peer: feat_copy(peer, slot).start())
        own_head.wait()
        for owner in range(last):
            head_copy(owner).wait_recv()
        in_group(lambda peer: feat_copy(peer, peer).wait_recv())
        columns[slot] = jnp.dot(
            feats[:, 0, :].astype(bf16), heads[...], preferred_element_type=f32
        )
        in_group(lambda peer: col_copy(peer, slot).start())
        arrived(texts, text_send, text_recv, "dp", replica, replicas)
        all_text = texts[:, 0, 0:span]
        label_column = texts[:, 0, span : span + 1]
        column = lax.broadcasted_iota(jnp.int32, (replicas, replicas), 1)
        targets = jnp.where(label_column == column.astype(f32), 1.0, 0.0)
        in_group(lambda peer: col_copy(peer, peer).wait_recv())
        embedding = jnp.concatenate([columns[index] for index in range(group)], axis=1)
        image_inv = lax.rsqrt(jnp.sum(embedding * embedding, axis=-1, keepdims=True) + epsilon)
        image_unit = embedding * image_inv
        member = lax.broadcasted_iota(jnp.int32, (group, 1), 0)
        if replicas == group:
            all_image = image_unit
        else:
            images[replica] = jnp.sum(
                jnp.where(member == slot, image_unit, 0.0), axis=0, keepdims=True
            )
            exchange(images, image_send, image_recv, "dp", replica, replicas)
            arrived(images, image_send, image_recv, "dp", replica, replicas)
            all_image = images[:, 0, :]
        logits = logit_scale * lax.dot_general(
            all_image,
            all_text,
            (((1,), (1,)), ((), ())),
            precision=lax.Precision.HIGHEST,
            preferred_element_type=f32,
        )
        row_max = jnp.max(logits, axis=1, keepdims=True)
        row_lse = row_max + jnp.log(jnp.sum(jnp.exp(logits - row_max), axis=1, keepdims=True))
        col_max = jnp.max(logits, axis=0, keepdims=True)
        col_lse = col_max + jnp.log(jnp.sum(jnp.exp(logits - col_max), axis=0, keepdims=True))
        d_logits = 0.5 * (
            (jnp.exp(logits - row_lse) - targets) + (jnp.exp(logits - col_lse) - targets)
        )
        if replicas != group:
            pick_row = lax.broadcasted_iota(jnp.int32, (group, replicas), 0) + first
            pick_column = lax.broadcasted_iota(jnp.int32, (group, replicas), 1)
            d_logits = jnp.dot(
                jnp.where(pick_row == pick_column, 1.0, 0.0),
                d_logits,
                precision=lax.Precision.HIGHEST,
                preferred_element_type=f32,
            )
        d_image = logit_scale * jnp.dot(
            d_logits, all_text, precision=lax.Precision.HIGHEST, preferred_element_type=f32
        )
        along = jnp.sum(d_image * image_unit, axis=-1, keepdims=True)
        d_rows[...] = (d_image - image_unit * along) * image_inv
        partial = lax.dot_general(
            d_rows[:, my_columns].astype(bf16),
            heads[...],
            (((1,), (1,)), ((), ())),
            preferred_element_type=f32,
        )
        for index in range(group):
            part_out[index] = partial[index : index + 1, :]
        in_group(lambda peer: part_copy(peer, slot).start())
        part_in[slot] = jnp.sum(jnp.where(member == slot, partial, 0.0), axis=0, keepdims=True)
        picked = jnp.sum(logits * targets, axis=1, keepdims=True)
        col_picked = jnp.sum(col_lse * targets, axis=1, keepdims=True)
        loss = 0.5 * (row_lse - picked) + 0.5 * (col_picked - picked)
        loss_ref[...] = jnp.broadcast_to(
            jnp.sum(loss, axis=0, keepdims=True) / replicas, loss_ref.shape
        )
        in_group(lambda peer: part_copy(peer, peer).wait_recv())
        d_std = jnp.sum(part_in[...], axis=0) * gain_ref[...]
        d_pooled = pooled_inv * (
            d_std
            - jnp.sum(d_std, axis=-1, keepdims=True) / width
            - pooled_std * (jnp.sum(d_std * pooled_std, axis=-1, keepdims=True) / width)
        )
        block[...] = jnp.broadcast_to((d_pooled / tokens).astype(bf16), block.shape)
        fill_grad.start()
        fill_grad.wait()
        in_group(lambda peer: feat_copy(peer, peer).wait_send())
        in_group(lambda peer: col_copy(peer, peer).wait_send())
        in_group(lambda peer: part_copy(peer, peer).wait_send())
        sent(texts, text_send, text_recv, "dp", replica, replicas)
        if replicas != group:
            sent(images, image_send, image_recv, "dp", replica, replicas)

    @pl.when(section < last)
    def _():
        head_copy(section).wait_send()

    def drain(index, carry):
        @pl.when(section < last)
        def _():
            forward_copy(index).wait_send()
            backward_copy(index).wait_recv()

        @pl.when(section > 0)
        def _():
            forward_copy(index).wait_recv()
            backward_copy(index).wait_send()

        return carry

    lax.fori_loop(0, shards, drain, 0)


def local(
    activations,
    saved,
    cotangents,
    projection,
    section_gain,
    final_gain,
    head_weight,
    text_embed,
    labels,
):
    sections, replicas = lax.axis_size("section"), lax.axis_size("dp")
    tokens, width = activations.shape[2:]
    rows, span = head_weight.shape
    group = math.gcd(replicas, span // 128)
    shard = span // group
    chunk = 256 if width % 256 == 0 else 128
    shards = width // chunk
    label_row = jnp.broadcast_to(labels.astype(jnp.float32)[:, None], (1, 128))
    f32, bf16 = jnp.float32, jnp.bfloat16
    dma = pltpu.SemaphoreType.DMA
    vmem = pl.BlockSpec(memory_space=pltpu.VMEM)
    whole = pl.BlockSpec(memory_space=pl.ANY)
    next_act, next_grad, loss_row = pl.pallas_call(
        functools.partial(step_kernel, sections, replicas, group, chunk),
        out_shape=(
            jax.ShapeDtypeStruct((tokens, width), bf16),
            jax.ShapeDtypeStruct((tokens, width), bf16),
            jax.ShapeDtypeStruct((1, 128), f32),
        ),
        in_specs=[whole] * 5 + [vmem] * 4,
        out_specs=(whole, whole, vmem),
        scratch_shapes=[
            pltpu.VMEM((tokens, width), bf16),
            pltpu.VMEM((tokens, width), bf16),
            pltpu.VMEM((tokens, width), bf16),
            pltpu.VMEM((width, width), bf16),
            pltpu.VMEM((tokens, width), bf16),
            pltpu.VMEM((tokens, width), bf16),
            pltpu.VMEM((tokens, width), bf16),
            pltpu.VMEM((tokens, width), f32),
            pltpu.VMEM((1, width), f32),
            pltpu.VMEM((sections * rows, shard), bf16),
            pltpu.VMEM((group, 1, width), f32),
            pltpu.VMEM((group, group, shard), f32),
            pltpu.VMEM((replicas, 1, span), f32),
            pltpu.VMEM((replicas, 1, span + 128), f32),
            pltpu.VMEM((group, span), f32),
            pltpu.VMEM((group, 1, width), f32),
            pltpu.VMEM((group, 1, width), f32),
            dma((3,)),
            dma((shards,)),
            dma,
            dma((sections,)),
            dma((shards,)),
            dma((shards,)),
            dma((shards,)),
            dma((shards,)),
            dma,
            dma((group,)),
            dma((group,)),
            dma((group,)),
            dma((group,)),
            dma((replicas,)),
            dma((replicas,)),
            dma((replicas,)),
            dma((replicas,)),
            dma((group,)),
            dma((group,)),
        ],
        compiler_params=pltpu.CompilerParams(collective_id=0, has_side_effects=True),
        name="tower_step",
    )(
        activations[0, 0],
        saved[0, 0],
        cotangents[0, 0],
        projection[0],
        head_weight,
        section_gain,
        final_gain[None],
        text_embed,
        label_row,
    )
    return (next_act[None, None], next_grad[None, None], loss_row[0, :1])


def solution(mesh):
    return jax.shard_map(
        local,
        mesh=mesh,
        in_specs=(
            P("section", "dp", None, None),
            P("section", "dp", None, None),
            P("section", "dp", None, None),
            P("section", None, None),
            P("section", None),
            P(),
            P("section", None),
            P("dp", None),
            P("dp"),
        ),
        out_specs=(P("section", "dp", None, None), P("section", "dp", None, None), P("section")),
        check_vma=False,
    )
```

```python
import functools
import math

import jax
import jax.numpy as jnp
from jax import lax
from jax.experimental import pallas as pl
from jax.experimental.pallas import tpu as pltpu
from jax.sharding import PartitionSpec as P

epsilon = 1e-06
logit_scale = 100.0
MESH = pl.DeviceIdType.MESH


def exchange(slots, send, recv, axis, me, peers):
    def start(step, carry):
        peer = lax.rem(me + step, peers)
        pltpu.make_async_remote_copy(
            slots.at[me], slots.at[me], send.at[peer], recv.at[me], {axis: peer}, MESH
        ).start()
        return carry

    lax.fori_loop(1, peers, start, 0)


def arrived(slots, send, recv, axis, me, peers):
    def wait(step, carry):
        peer = lax.rem(me + step, peers)
        pltpu.make_async_remote_copy(
            slots.at[me], slots.at[peer], send.at[peer], recv.at[peer], {axis: peer}, MESH
        ).wait_recv()
        return carry

    lax.fori_loop(1, peers, wait, 0)


def sent(slots, send, recv, axis, me, peers):
    def wait(step, carry):
        peer = lax.rem(me + step, peers)
        pltpu.make_async_remote_copy(
            slots.at[me], slots.at[me], send.at[peer], recv.at[peer], {axis: peer}, MESH
        ).wait_send()
        return carry

    lax.fori_loop(1, peers, wait, 0)


def enter(sections, replicas):
    section, replica = lax.axis_index("section"), lax.axis_index("dp")
    barrier = pltpu.get_barrier_semaphore()

    def greet_section(step, carry):
        peer = lax.rem(section + step, sections)
        pl.semaphore_signal(barrier, inc=1, device_id={"section": peer}, device_id_type=MESH)
        return carry

    def greet_replica(step, carry):
        peer = lax.rem(replica + step, replicas)
        pl.semaphore_signal(barrier, inc=1, device_id={"dp": peer}, device_id_type=MESH)
        return carry

    lax.fori_loop(1, sections, greet_section, 0)
    lax.fori_loop(1, replicas, greet_replica, 0)
    pl.semaphore_wait(barrier, sections + replicas - 2)


def row_stats(values):
    width = values.shape[-1]
    centre = jnp.sum(values, axis=-1, keepdims=True) / width
    centred = values - centre
    variance = jnp.sum(centred * centred, axis=-1, keepdims=True) / width
    return centre, lax.rsqrt(variance + epsilon)


def step_kernel(
    sections,
    replicas,
    group,
    chunk,
    act_ref,
    saved_ref,
    cot_ref,
    weight_ref,
    head_ref,
    scale_ref,
    gain_ref,
    text_ref,
    label_ref,
    next_ref,
    grad_ref,
    row_ref,
    loss_ref,
    act,
    saved,
    cot,
    weight,
    normed,
    block,
    d_input,
    slope,
    pooled,
    heads,
    feats,
    columns,
    images,
    texts,
    d_rows,
    part_out,
    part_in,
    relay,
    load_sem,
    weight_sem,
    head_send,
    head_recv,
    fwd_send,
    fwd_recv,
    bwd_send,
    bwd_recv,
    feat_send,
    feat_recv,
    col_send,
    col_recv,
    image_send,
    image_recv,
    text_send,
    text_recv,
    part_send,
    part_recv,
    relay_recv,
    pass_send,
):
    section, replica = lax.axis_index("section"), lax.axis_index("dp")
    last = sections - 1
    tokens, width = act.shape
    rows, span = head_ref.shape
    shards = width // chunk
    slot = lax.rem(replica, group)
    first = replica - slot
    shard = span // group
    f32, bf16 = jnp.float32, jnp.bfloat16

    def cut(index):
        return pl.ds(pl.multiple_of(index * chunk, chunk), chunk)

    def weight_load(index):
        return pltpu.make_async_copy(
            weight_ref.at[:, cut(index)], weight.at[:, cut(index)], weight_sem.at[index]
        )

    load_act = pltpu.make_async_copy(act_ref, act, load_sem.at[0])
    load_saved = pltpu.make_async_copy(saved_ref, saved, load_sem.at[1])
    load_cot = pltpu.make_async_copy(cot_ref, cot, load_sem.at[2])
    load_act.start()
    for index in range(shards):
        weight_load(index).start()
    load_saved.start()
    load_cot.start()
    enter(sections, replicas)

    my_columns = pl.ds(pl.multiple_of(slot * shard, shard), shard)

    def head_rows(owner):
        return pl.ds(pl.multiple_of(owner * rows, rows), rows)

    def head_copy(owner):
        return pltpu.make_async_remote_copy(
            head_ref.at[:, my_columns],
            heads.at[head_rows(owner), :],
            head_send,
            head_recv.at[owner],
            {"section": last},
            MESH,
        )

    own_head = pltpu.make_async_copy(
        head_ref.at[:, my_columns], heads.at[head_rows(last), :], head_send
    )

    @pl.when(section < last)
    def _():
        head_copy(section).start()

    @pl.when(section == last)
    def _():
        own_head.start()
        text = text_ref[...].astype(f32)
        text_inv = lax.rsqrt(jnp.sum(text * text, axis=-1, keepdims=True) + epsilon)
        texts[replica, :, 0:span] = text * text_inv
        texts[replica, :, span:] = jnp.full((1, 128), label_ref[0]).astype(f32)
        exchange(texts, text_send, text_recv, "dp", replica, replicas)

    cutoff = tokens // 2 // 16 * 16
    halves = (pl.ds(0, cutoff), pl.ds(cutoff, tokens - cutoff))

    def move(source, target, send, recv, peer, half, index):
        part = (halves[half], cut(index))
        return pltpu.make_async_remote_copy(
            source.at[part],
            target.at[part],
            send.at[half, index],
            recv.at[half, index],
            {"section": peer},
            MESH,
        )

    def forward_copy(half, index):
        return move(block, next_ref, fwd_send, fwd_recv, section + 1, half, index)

    def backward_copy(half, index):
        return move(d_input, grad_ref, bwd_send, bwd_recv, section - 1, half, index)

    middle = sections // 2
    relays = sections >= 4
    forward_relay, backward_relay = middle + 1, middle - 2

    def forward_detour(index):
        return move(block, relay, fwd_send, relay_recv, forward_relay, 1, index)

    def backward_detour(index):
        return move(d_input, relay, bwd_send, relay_recv, backward_relay, 1, index)

    def forward_pass(index):
        return move(relay, next_ref, pass_send, fwd_recv, middle, 1, index)

    def backward_pass(index):
        return move(relay, grad_ref, pass_send, bwd_recv, middle - 1, 1, index)

    def send_piece(direct, detour, origin, index):
        direct(0, index).start()
        if not relays:
            direct(1, index).start()
            return

        @pl.when(section == origin)
        def _():
            detour(index).start()

        @pl.when(section != origin)
        def _():
            direct(1, index).start()

    def send_forward(index):
        send_piece(forward_copy, forward_detour, middle - 1, index)

    def send_backward(index):
        send_piece(backward_copy, backward_detour, middle, index)

    def relay_all(detour, onward):
        def go(index, carry):
            detour(index).wait_recv()
            onward(index).start()
            return carry

        lax.fori_loop(0, shards, go, 0)

    def forward_step(index, carry):
        @pl.when(section < last)
        def _():
            weight_load(index).wait()

        mixed = jnp.dot(normed[...], weight[:, cut(index)], preferred_element_type=f32)
        piece = (act[:, cut(index)].astype(f32) + mixed).astype(bf16)
        block[:, cut(index)] = piece
        pooled[:, cut(index)] = jnp.sum(piece.astype(f32), axis=0, keepdims=True) / tokens

        @pl.when(section < last)
        def _():
            send_forward(index)

        return carry

    def forward():
        load_act.wait()
        values = act[...].astype(f32)
        centre, inverse = row_stats(values)
        normed[...] = ((values - centre) * inverse * scale_ref[...]).astype(bf16)
        lax.fori_loop(0, shards, forward_step, 0)

    def backward():
        load_saved.wait()
        load_cot.wait()
        centre, inverse = row_stats(saved[...].astype(f32))

        def gradient_step(index, carry):
            sum_slope, sum_product = carry
            d_normed = lax.dot_general(
                cot[...],
                weight[cut(index), :],
                (((1,), (1,)), ((), ())),
                preferred_element_type=f32,
            )
            piece = d_normed * scale_ref[:, cut(index)]
            standard = (saved[:, cut(index)].astype(f32) - centre) * inverse
            slope[:, cut(index)] = piece
            return (
                sum_slope + jnp.sum(piece, axis=-1, keepdims=True),
                sum_product + jnp.sum(piece * standard, axis=-1, keepdims=True),
            )

        zero = jnp.zeros((tokens, 1), f32)
        sum_slope, sum_product = lax.fori_loop(0, shards, gradient_step, (zero, zero))
        mean_slope, mean_product = sum_slope / width, sum_product / width

        def emit_step(index, carry):
            standard = (saved[:, cut(index)].astype(f32) - centre) * inverse
            d_input[:, cut(index)] = (
                cot[:, cut(index)].astype(f32)
                + inverse * (slope[:, cut(index)] - mean_slope - standard * mean_product)
            ).astype(bf16)
            send_backward(index)
            return carry

        lax.fori_loop(0, shards, emit_step, 0)

    @pl.when(section == last)
    def _():
        for index in range(shards):
            weight_load(index).wait()
        backward()

    forward()

    @pl.when((section > 0) & (section < last))
    def _():
        backward()

    @pl.when(section == 0)
    def _():
        load_saved.wait()
        load_cot.wait()

    loss_ref[...] = jnp.zeros_like(loss_ref)
    row_ref[...] = jnp.zeros_like(row_ref)

    if relays:

        @pl.when(section == forward_relay)
        def _():
            relay_all(forward_detour, forward_pass)

        @pl.when(section == backward_relay)
        def _():
            relay_all(backward_detour, backward_pass)

    @pl.when(section == last)
    def _():
        mean_row = pooled[...]
        centre, pooled_inv = row_stats(mean_row)
        pooled_std = (mean_row - centre) * pooled_inv
        feats[slot] = (pooled_std * gain_ref[...].reshape(1, width)).astype(bf16).astype(f32)

        def in_group(make):
            def go(step, carry):
                peer = lax.rem(slot + step, group)
                make(peer)
                return carry

            lax.fori_loop(1, group, go, 0)

        def feat_copy(peer, source):
            return pltpu.make_async_remote_copy(
                feats.at[slot],
                feats.at[source],
                feat_send.at[peer],
                feat_recv.at[source],
                {"dp": first + peer},
                MESH,
            )

        def col_copy(peer, source):
            return pltpu.make_async_remote_copy(
                columns.at[slot],
                columns.at[source],
                col_send.at[peer],
                col_recv.at[source],
                {"dp": first + peer},
                MESH,
            )

        def part_copy(peer, source):
            return pltpu.make_async_remote_copy(
                part_out.at[peer],
                part_in.at[source],
                part_send.at[peer],
                part_recv.at[source],
                {"dp": first + peer},
                MESH,
            )

        in_group(lambda peer: feat_copy(peer, slot).start())
        own_head.wait()
        for owner in range(last):
            head_copy(owner).wait_recv()
        in_group(lambda peer: feat_copy(peer, peer).wait_recv())
        columns[slot] = jnp.dot(
            feats[:, 0, :].astype(bf16), heads[...], preferred_element_type=f32
        )
        in_group(lambda peer: col_copy(peer, slot).start())
        arrived(texts, text_send, text_recv, "dp", replica, replicas)
        all_text = texts[:, 0, 0:span]
        label_column = texts[:, 0, span : span + 1]
        column = lax.broadcasted_iota(jnp.int32, (replicas, replicas), 1)
        targets = jnp.where(label_column == column.astype(f32), 1.0, 0.0)
        in_group(lambda peer: col_copy(peer, peer).wait_recv())
        embedding = jnp.concatenate([columns[index] for index in range(group)], axis=1)
        image_inv = lax.rsqrt(jnp.sum(embedding * embedding, axis=-1, keepdims=True) + epsilon)
        image_unit = embedding * image_inv
        member = lax.broadcasted_iota(jnp.int32, (group, 1), 0)
        if replicas == group:
            all_image = image_unit
        else:
            images[replica] = jnp.sum(
                jnp.where(member == slot, image_unit, 0.0), axis=0, keepdims=True
            )
            exchange(images, image_send, image_recv, "dp", replica, replicas)
            arrived(images, image_send, image_recv, "dp", replica, replicas)
            all_image = images[:, 0, :]
        logits = logit_scale * lax.dot_general(
            all_image,
            all_text,
            (((1,), (1,)), ((), ())),
            precision=lax.Precision.HIGHEST,
            preferred_element_type=f32,
        )
        row_max = jnp.max(logits, axis=1, keepdims=True)
        row_lse = row_max + jnp.log(jnp.sum(jnp.exp(logits - row_max), axis=1, keepdims=True))
        col_max = jnp.max(logits, axis=0, keepdims=True)
        col_lse = col_max + jnp.log(jnp.sum(jnp.exp(logits - col_max), axis=0, keepdims=True))
        d_logits = 0.5 * (
            (jnp.exp(logits - row_lse) - targets) + (jnp.exp(logits - col_lse) - targets)
        )
        if replicas != group:
            pick_row = lax.broadcasted_iota(jnp.int32, (group, replicas), 0) + first
            pick_column = lax.broadcasted_iota(jnp.int32, (group, replicas), 1)
            d_logits = jnp.dot(
                jnp.where(pick_row == pick_column, 1.0, 0.0),
                d_logits,
                precision=lax.Precision.HIGHEST,
                preferred_element_type=f32,
            )
        d_image = logit_scale * jnp.dot(
            d_logits, all_text, precision=lax.Precision.HIGHEST, preferred_element_type=f32
        )
        along = jnp.sum(d_image * image_unit, axis=-1, keepdims=True)
        d_rows[...] = (d_image - image_unit * along) * image_inv
        partial = lax.dot_general(
            d_rows[:, my_columns].astype(bf16),
            heads[...],
            (((1,), (1,)), ((), ())),
            preferred_element_type=f32,
        )
        for index in range(group):
            part_out[index] = partial[index : index + 1, :]
        in_group(lambda peer: part_copy(peer, slot).start())
        part_in[slot] = jnp.sum(jnp.where(member == slot, partial, 0.0), axis=0, keepdims=True)
        picked = jnp.sum(logits * targets, axis=1, keepdims=True)
        col_picked = jnp.sum(col_lse * targets, axis=1, keepdims=True)
        loss = 0.5 * (row_lse - picked) + 0.5 * (col_picked - picked)
        loss_ref[...] = jnp.broadcast_to(
            jnp.sum(loss, axis=0, keepdims=True) / replicas, loss_ref.shape
        )
        in_group(lambda peer: part_copy(peer, peer).wait_recv())
        d_std = jnp.sum(part_in[...], axis=0) * gain_ref[...].reshape(1, width)
        d_pooled = pooled_inv * (
            d_std
            - jnp.sum(d_std, axis=-1, keepdims=True) / width
            - pooled_std * (jnp.sum(d_std * pooled_std, axis=-1, keepdims=True) / width)
        )
        row_ref[...] = d_pooled / tokens
        in_group(lambda peer: feat_copy(peer, peer).wait_send())
        in_group(lambda peer: col_copy(peer, peer).wait_send())
        in_group(lambda peer: part_copy(peer, peer).wait_send())
        sent(texts, text_send, text_recv, "dp", replica, replicas)
        if replicas != group:
            sent(images, image_send, image_recv, "dp", replica, replicas)

    @pl.when(section < last)
    def _():
        head_copy(section).wait_send()

    def drain(index, carry):
        for half in range(2):

            @pl.when(section < last)
            def _():
                forward_copy(half, index).wait_send()
                backward_copy(half, index).wait_recv()

            @pl.when(section > 0)
            def _():
                forward_copy(half, index).wait_recv()
                backward_copy(half, index).wait_send()

        if relays:

            @pl.when((section == forward_relay) | (section == backward_relay))
            def _():
                forward_pass(index).wait_send()

        return carry

    lax.fori_loop(0, shards, drain, 0)


def local(
    activations,
    saved,
    cotangents,
    projection,
    section_gain,
    final_gain,
    head_weight,
    text_embed,
    labels,
):
    sections, replicas = lax.axis_size("section"), lax.axis_size("dp")
    tokens, width = activations.shape[2:]
    rows, span = head_weight.shape
    group = math.gcd(replicas, span // 128)
    shard = span // group
    chunk = 256 if width % 256 == 0 else 128
    shards = width // chunk
    f32, bf16 = jnp.float32, jnp.bfloat16
    dma = pltpu.SemaphoreType.DMA
    vmem = pl.BlockSpec(memory_space=pltpu.VMEM)
    whole = pl.BlockSpec(memory_space=pl.ANY)
    next_raw, grad_raw, grad_row, loss_row = pl.pallas_call(
        functools.partial(step_kernel, sections, replicas, group, chunk),
        out_shape=(
            jax.ShapeDtypeStruct((tokens, width), bf16),
            jax.ShapeDtypeStruct((tokens, width), bf16),
            jax.ShapeDtypeStruct((1, width), f32),
            jax.ShapeDtypeStruct((1, 128), f32),
        ),
        in_specs=[whole] * 5 + [vmem] * 3 + [pl.BlockSpec(memory_space=pltpu.SMEM)],
        out_specs=(whole, whole, vmem, vmem),
        scratch_shapes=[
            pltpu.VMEM((tokens, width), bf16),
            pltpu.VMEM((tokens, width), bf16),
            pltpu.VMEM((tokens, width), bf16),
            pltpu.VMEM((width, width), bf16),
            pltpu.VMEM((tokens, width), bf16),
            pltpu.VMEM((tokens, width), bf16),
            pltpu.VMEM((tokens, width), bf16),
            pltpu.VMEM((tokens, width), f32),
            pltpu.VMEM((1, width), f32),
            pltpu.VMEM((sections * rows, shard), bf16),
            pltpu.VMEM((group, 1, width), f32),
            pltpu.VMEM((group, group, shard), f32),
            pltpu.VMEM((replicas, 1, span), f32),
            pltpu.VMEM((replicas, 1, span + 128), f32),
            pltpu.VMEM((group, span), f32),
            pltpu.VMEM((group, 1, width), f32),
            pltpu.VMEM((group, 1, width), f32),
            pltpu.VMEM((tokens, width), bf16),
            dma((3,)),
            dma((shards,)),
            dma,
            dma((sections,)),
            dma((2, shards)),
            dma((2, shards)),
            dma((2, shards)),
            dma((2, shards)),
            dma((group,)),
            dma((group,)),
            dma((group,)),
            dma((group,)),
            dma((replicas,)),
            dma((replicas,)),
            dma((replicas,)),
            dma((replicas,)),
            dma((group,)),
            dma((group,)),
            dma((2, shards)),
            dma((2, shards)),
        ],
        compiler_params=pltpu.CompilerParams(collective_id=0, has_side_effects=True),
        name="tower_step",
    )(
        activations[0, 0],
        saved[0, 0],
        cotangents[0, 0],
        projection[0],
        head_weight,
        section_gain,
        final_gain,
        text_embed,
        labels,
    )
    section = lax.axis_index("section")
    next_act = jnp.where(section == 0, jnp.zeros_like(next_raw), next_raw)
    next_grad = jnp.where(section == sections - 1, grad_row.astype(bf16), grad_raw)
    return (next_act[None, None], next_grad[None, None], loss_row[0, :1])


def solution(mesh):
    return jax.shard_map(
        local,
        mesh=mesh,
        in_specs=(
            P("section", "dp", None, None),
            P("section", "dp", None, None),
            P("section", "dp", None, None),
            P("section", None, None),
            P("section", None),
            P(),
            P("section", None),
            P("dp", None),
            P("dp"),
        ),
        out_specs=(P("section", "dp", None, None), P("section", "dp", None, None), P("section")),
        check_vma=False,
    )
```
